32 devices in a mesh: dp: 2 (over core), expert: 16 (over z, y, x).
Axes of the slice: x: 2, y: 2, z: 4, core: 2. Of those that a mesh axis runs over, the one named last changes fastest.
Arguments:
- tokens: bfloat16 [8192, 1280], P(('dp', 'expert')), may hold values from -48 to 48
- phi: bfloat16 [1280, 48], replicated, may hold values from -0.05 to 0.05
- slot_count: int32 [16], replicated, may hold values from 1 to 3, 40 in all
- w_in: bfloat16 [16, 2560, 1280], P('expert'), may hold values from -1.25 to 1.25
- w_out: bfloat16 [16, 2560, 1280], P('expert'), may hold values from -1 to 1
- grad_out: bfloat16 [8192, 1280], P(('dp', 'expert')), may hold values from -6 to 6
Outputs:
- mixed_out: bfloat16 [8192, 1280], P(('dp', 'expert'))
- grad_tokens: bfloat16 [8192, 1280], P(('dp', 'expert'))
- grad_phi: float32 [1280, 48], replicated
- grad_w_in: bfloat16 [16, 2560, 1280], P('expert', 'dp')
- grad_w_out: bfloat16 [16, 2560, 1280], P('expert', 'dp')
The draws below stay inside these ranges and needn't reach their ends.
Inputs may be any that keep to these rules, and one draw needn't show every extreme that they name: slot_count sums to 40; some expert has exactly 3.
All inputs are finite; a program needn't handle non-finite values.
Results may differ from the reference program's by a relative error of at most 0.012.
The reference program's roundings to bfloat16 on the way count: a program that leaves them out, or rounds other values in their place, can miss the bound.
Values may be sent and summed in bfloat16 or wider, within the bound.
A program may use at most 128 MiB of HBM per device.

```python
import math
import jax
import jax.numpy as jnp
import numpy as np
from jax import lax

D = 1280
FF = 2560
TOK = 256
MOST = 3
EXPERTS = 16
SLOTS = 40
IMAGES = 32
TOKENS = 8192


def phi_entries(key):
    return jax.random.uniform(jax.random.fold_in(key, 11), (D, EXPERTS * MOST), jnp.float32, minval=-0.0495, maxval=0.0495)


def draw_phi(key, part):
    return phi_entries(key).astype(jnp.bfloat16)


def draw_tokens(key, part):
    samples = jax.random.normal(jax.random.fold_in(key, 23), (IMAGES, TOK, D), jnp.float32)
    return jnp.clip(samples, -48.0, 48.0).reshape(TOKENS, D).astype(jnp.bfloat16)


def block_levels(own_key, shape, cuts, least, high):
    def one(axis_at, blocks):
        draws = jax.random.uniform(jax.random.fold_in(jax.random.fold_in(own_key, 6), axis_at), (blocks,), jnp.float32, least / len(cuts), high / len(cuts))
        return jnp.repeat(jnp.exp(draws), shape[axis_at] // blocks).reshape((-1,) + (1,) * (len(shape) - axis_at - 1))

    level = one(*cuts[0])
    for cut in cuts[1:]:
        level = level * one(*cut)
    return level


def length_profile(amount, total, bound, skew):
    portions = [(1 << 20) // math.isqrt(grade ** skew) + 1 for grade in range(2, amount + 1)]
    rest, given = total - bound - (amount - 1), [1] * (amount - 1)
    while rest > 0:
        candidates = [i for i in range(amount - 1) if given[i] < bound]
        mass, left = sum([portions[i] for i in candidates]), rest
        for i in candidates:
            addition = min(bound - given[i], max(1, left * portions[i] // mass), rest)
            given[i] = given[i] + addition
            rest = rest - addition
    return np.array([bound] + given)


def ragged(rng, number_of, total, most, slope):
    if number_of == 2:
        one = jax.random.randint(rng, (), max(1, total - most), min(most, total - 1) + 1)
        return jnp.stack([one, total - one])
    lengths = jnp.asarray(length_profile(number_of, total, most, slope), jnp.int32)
    pairs = (number_of - 1) // 2
    source_of, sink = lengths[1:1 + 2 * pairs:2], lengths[2:2 + 2 * pairs:2]
    margin = jnp.minimum(source_of - 1, most - sink)
    passed = jax.random.randint(jax.random.fold_in(rng, 1), (pairs,), 0, 1 << 20) % (margin + 1)
    lengths = lengths.at[1:1 + 2 * pairs:2].set(source_of - passed).at[2:2 + 2 * pairs:2].set(sink + passed)
    return lengths[jax.random.permutation(jax.random.fold_in(rng, 2), number_of)]


def noise(rng, shape, scale, most, cuts=(), held_as=jnp.bfloat16):
    loudness = block_levels(rng, shape, cuts, -0.22, 0.18) if cuts else 1.0
    entries = jax.random.normal(rng, shape, jnp.float32) * scale * loudness
    return jnp.minimum(jnp.maximum(entries, -most), most).astype(held_as)


def setup_inputs(seed: int = 0) -> dict:
    key_list = jax.random.split(jax.random.key(seed), 7)
    tokens = draw_tokens(jax.random.fold_in(key_list[6], 71), 0)
    phi = draw_phi(jax.random.fold_in(key_list[6], 71), 0)
    slot_count = ragged(key_list[2], EXPERTS, SLOTS, MOST, 2).astype(jnp.int32)
    w_in = noise(key_list[3], (EXPERTS, FF, D), (max(D // 64, 4)) ** -0.5, 1.25, ((0, 16),))
    w_out = noise(key_list[4], (EXPERTS, FF, D), (max(FF // 64, 4)) ** -0.5, 1.0, ((0, 16),))
    grad_out = noise(key_list[5], (TOKENS, D), 1.0, 6.0, ((0, 32),))
    return {"tokens": tokens, "phi": phi, "slot_count": slot_count, "w_in": w_in, "w_out": w_out, "grad_out": grad_out}


SQRT_HALF = 0.7071067811865476
INV_SQRT_TAU = 0.3989422804014327


def contract(left, right, left_dim, right_dim):
    return lax.dot_general(left, right, (((left_dim,), (right_dim,)), ((), ())), preferred_element_type=jnp.float32)


def softmax_along(logits, axis):
    maximum = jnp.max(logits, axis=axis, keepdims=True)
    weights = jnp.exp(logits - maximum)
    return weights / jnp.sum(weights, axis=axis, keepdims=True)


def gelu_parts(preact):
    normal_cdf = 0.5 * (1.0 + jax.scipy.special.erf(preact * SQRT_HALF))
    density = jnp.exp(-0.5 * preact * preact) * INV_SQRT_TAU
    return preact * normal_cdf, normal_cdf + preact * density


def live_slots(slot_count):
    positions = lax.broadcasted_iota(jnp.int32, (slot_count.shape[0], MOST), 1)
    return (positions < slot_count[:, None]).reshape(-1)


def image_front(image_tokens, phi, live_mask):
    logits = jnp.dot(image_tokens, phi, preferred_element_type=jnp.float32)
    spread = softmax_along(logits, 0)
    spread_b = spread.astype(jnp.bfloat16)
    slot_in = contract(spread_b, image_tokens, 0, 0).astype(jnp.bfloat16)
    mixing = softmax_along(jnp.where(live_mask[None, :], logits, -1e30), 1)
    return slot_in, spread, spread_b, mixing


def image_returned(image_tokens, phi, output_cotangent, slot_values, slot_grads, spread, spread_b, mixing):
    d_mix = contract(output_cotangent, slot_values, 1, 1)
    d_comb = mixing * (d_mix - jnp.sum(d_mix * mixing, axis=1, keepdims=True))
    d_spread = contract(image_tokens, slot_grads, 1, 1)
    d_disp = spread * (d_spread - jnp.sum(d_spread * spread, axis=0, keepdims=True))
    d_logits = (d_comb + d_disp).astype(jnp.bfloat16)
    image_gradient = contract(d_logits, phi, 1, 1) + jnp.dot(spread_b, slot_grads, preferred_element_type=jnp.float32)
    return image_gradient.astype(jnp.bfloat16), contract(image_tokens, d_logits, 0, 0)


def expert_front(slot_rows, first_proj, second_proj):
    preact = contract(slot_rows, first_proj, 1, 1)
    activated, slopes = gelu_parts(preact)
    hidden = activated.astype(jnp.bfloat16)
    return jnp.dot(hidden, second_proj, preferred_element_type=jnp.float32), hidden, slopes


def expert_back(slot_rows, hidden, slopes, row_grads, first_proj, second_proj):
    d_hidden = contract(row_grads, second_proj, 1, 1)
    grad_pre = (d_hidden * slopes).astype(jnp.bfloat16)
    grad_rows = jnp.dot(grad_pre, first_proj, preferred_element_type=jnp.float32)
    grad_first = contract(grad_pre, slot_rows, 0, 0)
    grad_second = contract(hidden, row_grads, 0, 0)
    return grad_rows, grad_first, grad_second


def to_experts(array):
    return array.reshape(IMAGES, EXPERTS, MOST, D).transpose(1, 0, 2, 3).reshape(EXPERTS, IMAGES * MOST, D)


def to_images(array):
    return array.reshape(EXPERTS, IMAGES, MOST, D).transpose(1, 0, 2, 3).reshape(IMAGES, EXPERTS * MOST, D)


def reference(tokens, phi, slot_count, w_in, w_out, grad_out):
    live_mask = live_slots(slot_count)
    images = tokens.reshape(IMAGES, TOK, D)
    cotangents = grad_out.reshape(IMAGES, TOK, D)

    def front(packed_group):
        image_tokens, output_cotangent = packed_group
        slot_in, spread, spread_b, mixing = image_front(image_tokens, phi, live_mask)
        mixing_b = mixing.astype(jnp.bfloat16)
        slot_cot = contract(mixing_b, output_cotangent, 0, 0).astype(jnp.bfloat16)
        return slot_in, slot_cot, spread, spread_b, mixing, mixing_b

    slot_in, slot_cot, spread, spread_b, mixing, mixing_b = lax.map(front, (images, cotangents))

    def expert(packed_group):
        slot_rows, row_grads, first_proj, second_proj = packed_group
        values, hidden, slopes = expert_front(slot_rows, first_proj, second_proj)
        grad_rows, grad_first, grad_second = expert_back(slot_rows, hidden, slopes, row_grads, first_proj, second_proj)
        return (values.astype(jnp.bfloat16), grad_rows.astype(jnp.bfloat16),
                grad_first.astype(jnp.bfloat16), grad_second.astype(jnp.bfloat16))

    values, grad_rows, grad_w_in, grad_w_out = lax.map(expert, (to_experts(slot_in), to_experts(slot_cot), w_in, w_out))
    slot_values = to_images(values)
    slot_grads = to_images(grad_rows)

    def back(packed_group):
        image_tokens, output_cotangent, slot_state, slot_gradient, dispatch_weight, dispatch_weight_batch, combine_weight, combine_weight_batch = packed_group
        combined_output = jnp.dot(combine_weight_batch, slot_state, preferred_element_type=jnp.float32).astype(jnp.bfloat16)
        image_gradient, gradient_piece = image_returned(image_tokens, phi, output_cotangent, slot_state, slot_gradient, dispatch_weight, dispatch_weight_batch, combine_weight)
        return combined_output, image_gradient, gradient_piece

    combined_output, grad_images, grad_terms = lax.map(back, (images, cotangents, slot_values, slot_grads, spread, spread_b, mixing, mixing_b))
    grad_phi = jnp.sum(grad_terms, axis=0)
    return combined_output.reshape(TOKENS, D), grad_images.reshape(TOKENS, D), grad_phi, grad_w_in, grad_w_out
```

```python
import functools

import jax
import jax.numpy as jnp
from jax import lax
from jax.experimental import pallas as pl
from jax.experimental.pallas import tpu as pltpu
from jax.sharding import PartitionSpec as P

LANES = 128
TILE = 16
SQRT_HALF = 0.7071067811865476
INV_SQRT_TAU = 0.3989422804014327
MESH = pl.DeviceIdType.MESH
BF16 = jnp.bfloat16
F32 = jnp.float32


def contract(left, right, left_dim, right_dim):
    return lax.dot_general(
        left, right, (((left_dim,), (right_dim,)), ((), ())), preferred_element_type=F32
    )


def softmax_along(logits, axis):
    maximum = jnp.max(logits, axis=axis, keepdims=True)
    weights = jnp.exp(logits - maximum)
    return weights / jnp.sum(weights, axis=axis, keepdims=True)


def kernel(
    dims,
    count_ref, x_hbm, phi_hbm, g_hbm, win_hbm, wout_hbm,
    mixed_hbm, gtok_hbm, gphi_hbm, gwin_hbm, gwout_hbm,
    x_v, phi_v, g_v, win_v, wout_v,
    slot_f, pack_f, send_b, recv_b,
    rows_b, cots_b, hid_b, pre_b, slope_f,
    slots_v, mixed_v, gtok_v, gphi_f, gphi_v, gwin_v, gwout_v,
    rs_f, rs_send, rs_recv, ag_own, ag_recv,
    load_sem, store_sem, swap_send, swap_recv, send_sem, recv_sem,
):
    n_dp, experts, most, blocks, msg, piece = dims
    my_dp = lax.axis_index("dp")
    me = lax.axis_index("expert")
    flat = my_dp * experts + me
    n_all = n_dp * experts
    rows = experts * most
    half = win_v.shape[0] // n_dp
    share = blocks // n_dp

    def lane(k):
        return slice(k * LANES, (k + 1) * LANES)

    def load(src, dst, i):
        return pltpu.make_async_copy(src, dst, load_sem.at[i])

    x_in, phi_in, g_in = load(x_hbm, x_v, 0), load(phi_hbm, phi_v, 1), load(g_hbm, g_v, 2)
    win_in, wout_in = load(win_hbm.at[0], win_v, 3), load(wout_hbm.at[0], wout_v, 4)
    x_in.start()
    phi_in.start()
    g_in.start()

    barrier = pltpu.get_barrier_semaphore()

    @pl.loop(1, n_all)
    def _(t):
        to = lax.rem(flat + t, n_all)
        pl.semaphore_signal(
            barrier, inc=1, device_id=(lax.div(to, experts), lax.rem(to, experts)),
            device_id_type=MESH,
        )

    pack_f[...] = jnp.zeros_like(pack_f)
    rs_f[...] = jnp.zeros_like(rs_f)

    def to_experts(phase):
        for k in range(blocks):
            for j in range(most):
                pack_f[pl.ds(j * blocks + k, experts, stride=msg), :] = slot_f[
                    k, pl.ds(j, experts, stride=most), :
                ]
        ship(phase)

    def to_images(phase, values):
        for k in range(blocks):
            for j in range(most):
                pack_f[pl.ds(j * blocks + k, experts, stride=msg), :] = values[
                    j * experts:(j + 1) * experts, lane(k)
                ]
        ship(phase)

    def ship(phase):
        send_b[phase] = pack_f[...].astype(BF16).reshape(experts, msg, LANES)
        recv_b[phase, me] = send_b[phase, me]

        @pl.loop(1, experts)
        def _(t):
            to = lax.rem(me + t, experts)
            pltpu.make_async_remote_copy(
                src_ref=send_b.at[phase, to],
                dst_ref=recv_b.at[phase, me],
                send_sem=send_sem.at[phase],
                recv_sem=recv_sem.at[phase],
                device_id=(my_dp, to),
                device_id_type=MESH,
            ).start()

    def wait_bytes(ref, sem):
        pltpu.make_async_copy(ref, ref, sem).wait()

    def arrive(phase):
        wait_bytes(recv_b.at[phase, pl.ds(0, experts - 1)], recv_sem.at[phase])
        pack_f[...] = recv_b[phase].astype(F32).reshape(experts * msg, LANES)

    def at_expert(phase, dst):
        arrive(phase)
        for k in range(blocks):
            for j in range(most):
                dst[j * experts:(j + 1) * experts, lane(k)] = pack_f[
                    pl.ds(j * blocks + k, experts, stride=msg), :
                ].astype(BF16)

    def at_image(phase, which):
        arrive(phase)
        for k in range(blocks):
            for j in range(most):
                slot_f[k, pl.ds(j, experts, stride=most), :] = pack_f[
                    pl.ds(j * blocks + k, experts, stride=msg), :
                ]
            slots_v[which, :, lane(k)] = slot_f[k].astype(BF16)

    column = lax.broadcasted_iota(jnp.int32, (1, rows), 1)
    limit = jnp.zeros((1, rows), jnp.int32)
    for e in range(experts):
        limit = jnp.where(column >= e * most, e * most + count_ref[e], limit)
    live = column < limit

    x_in.wait()
    phi_in.wait()
    x = x_v[...]
    logits = jnp.dot(x, phi_v[...], preferred_element_type=F32)
    spread = softmax_along(logits, 0)
    spread_b = spread.astype(BF16)
    slot_in = contract(spread_b, x, 0, 0)
    for k in range(blocks):
        slot_f[k] = slot_in[:, lane(k)]
    pl.semaphore_wait(barrier, n_all - 1)
    to_experts(0)

    g_in.wait()
    win_in.start()
    wout_in.start()
    mixing = softmax_along(jnp.where(live, logits, -1e30), 1)
    mixing_b = mixing.astype(BF16)
    slot_cot = contract(mixing_b, g_v[...], 0, 0)
    for k in range(blocks):
        slot_f[k] = slot_cot[:, lane(k)]
    to_experts(1)

    win_in.wait()
    at_expert(0, rows_b)
    wout_in.wait()
    slot_rows = rows_b[...]
    values = None
    for h in range(n_dp):
        span = slice(h * half, (h + 1) * half)
        preact = contract(slot_rows, win_v[span], 1, 1)
        cdf = 0.5 * (1.0 + lax.erf(preact * SQRT_HALF))
        density = jnp.exp(-0.5 * preact * preact) * INV_SQRT_TAU
        hidden = (preact * cdf).astype(BF16)
        slope_f[h] = cdf + preact * density
        hid_b[h] = hidden
        part = jnp.dot(hidden, wout_v[span], preferred_element_type=F32)
        values = part if values is None else values + part
    to_images(2, values)

    at_expert(1, cots_b)
    cot_rows = cots_b[...]
    grads = None
    for h in range(n_dp):
        span = slice(h * half, (h + 1) * half)
        d_hidden = contract(cot_rows, wout_v[span], 1, 1)
        grad_pre = (d_hidden * slope_f[h]).astype(BF16)
        pre_b[h] = grad_pre
        part = jnp.dot(grad_pre, win_v[span], preferred_element_type=F32)
        grads = part if grads is None else grads + part
    to_images(3, grads)

    other = 1 - my_dp

    def swap(src, dst, i):
        return pltpu.make_async_remote_copy(
            src_ref=src, dst_ref=dst, send_sem=swap_send.at[i], recv_sem=swap_recv.at[i],
            device_id=(other, me), device_id_type=MESH,
        )

    swaps = (
        swap(hid_b.at[other], hid_b.at[n_dp], 0),
        swap(pre_b.at[other], pre_b.at[n_dp], 1),
        swap(rows_b, slots_v.at[2], 2),
        swap(cots_b, slots_v.at[3], 3),
    )
    for copy in swaps:
        copy.start()

    at_image(2, 0)
    slot_values = slots_v[0]
    d_mix = contract(g_v[...], slot_values, 1, 1)
    d_comb = mixing * (d_mix - jnp.sum(d_mix * mixing, axis=1, keepdims=True))
    mixed_v[...] = jnp.dot(mixing_b, slot_values, preferred_element_type=F32).astype(BF16)

    def store(src, dst, i):
        return pltpu.make_async_copy(src, dst, store_sem.at[i])

    mixed_out = store(mixed_v, mixed_hbm, 0)
    mixed_out.start()

    for copy in swaps:
        copy.wait()
    outs = []
    for i, (left, right, theirs, buf, out) in enumerate((
        (pre_b, rows_b, slots_v.at[2], gwin_v, gwin_hbm),
        (hid_b, cots_b, slots_v.at[3], gwout_v, gwout_hbm),
    )):
        mine, given = left[my_dp], left[n_dp]
        buf[...] = (
            contract(mine, right[...], 0, 0) + contract(given, theirs[...], 0, 0)
        ).astype(BF16)
        outs.append(store(buf, out.at[0], 3 + i))
        outs[-1].start()

    at_image(3, 1)
    slot_grads = slots_v[1]
    d_spread = contract(x_v[...], slot_grads, 1, 1)
    d_disp = spread * (d_spread - jnp.sum(d_spread * spread, axis=0, keepdims=True))
    d_logits = (d_comb + d_disp).astype(BF16)
    term = contract(d_logits, x_v[...], 0, 0)

    for k in range(blocks):
        slot_f[k] = term[:, lane(k)]
    for k in range(blocks):
        for j in range(most):
            rs_f[k // share, pl.ds(j * share + k % share, experts, stride=piece), :] = slot_f[
                k, pl.ds(j, experts, stride=most), :
            ]
    rs_send[...] = rs_f[...].astype(BF16).reshape(n_all, piece, LANES)
    rs_recv[flat] = rs_send[flat]

    def to_all(src_of, dst, i):
        @pl.loop(1, n_all)
        def _(t):
            to = lax.rem(flat + t, n_all)
            pltpu.make_async_remote_copy(
                src_ref=src_of(to), dst_ref=dst.at[flat],
                send_sem=send_sem.at[i], recv_sem=recv_sem.at[i],
                device_id=(lax.div(to, experts), lax.rem(to, experts)),
                device_id_type=MESH,
            ).start()

    to_all(lambda to: rs_send.at[to], rs_recv, 4)

    gtok_v[...] = (
        contract(d_logits, phi_v[...], 1, 1)
        + jnp.dot(spread_b, slot_grads, preferred_element_type=F32)
    ).astype(BF16)
    gtok_out = store(gtok_v, gtok_hbm, 1)
    gtok_out.start()

    wait_bytes(rs_recv.at[pl.ds(0, n_all - 1)], recv_sem.at[4])
    ag_own[...] = jnp.sum(rs_recv[...].astype(F32), axis=0).astype(BF16)
    ag_recv[flat] = ag_own[...]
    to_all(lambda to: ag_own, ag_recv, 5)
    wait_bytes(ag_recv.at[pl.ds(0, n_all - 1)], recv_sem.at[5])
    rs_f[...] = ag_recv[...].astype(F32).reshape(n_dp, experts * piece, LANES)
    for k in range(blocks):
        for j in range(most):
            gphi_f[k, pl.ds(j, experts, stride=most), :] = rs_f[
                k // share, pl.ds(j * share + k % share, experts, stride=piece), :
            ]
        gphi_v[lane(k), :] = gphi_f[k].T
    gphi_out = store(gphi_v, gphi_hbm, 2)
    gphi_out.start()

    for phase in range(4):
        wait_bytes(send_b.at[phase, pl.ds(0, experts - 1)], send_sem.at[phase])
    wait_bytes(rs_send.at[pl.ds(0, n_all - 1)], send_sem.at[4])
    wait_bytes(ag_recv.at[pl.ds(0, n_all - 1)], send_sem.at[5])
    for copy in (mixed_out, gtok_out, *outs, gphi_out):
        copy.wait()


def local(n_dp, tokens, phi, slot_count, w_in, w_out, grad_out):
    experts = slot_count.shape[0]
    count, width = tokens.shape
    units = w_in.shape[1]
    rows = phi.shape[1]
    most = rows // experts
    blocks = width // LANES
    msg = -(-most * blocks // TILE) * TILE
    piece = -(-most * (blocks // n_dp) // TILE) * TILE
    half = units // n_dp
    n_all = n_dp * experts
    dims = (n_dp, experts, most, blocks, msg, piece)
    anywhere = pl.BlockSpec(memory_space=pl.ANY)
    vmem = pltpu.VMEM
    return pl.pallas_call(
        functools.partial(kernel, dims),
        out_shape=(
            jax.ShapeDtypeStruct((count, width), BF16),
            jax.ShapeDtypeStruct((count, width), BF16),
            jax.ShapeDtypeStruct((width, rows), F32),
            jax.ShapeDtypeStruct((1, half, width), BF16),
            jax.ShapeDtypeStruct((1, half, width), BF16),
        ),
        in_specs=[pl.BlockSpec(memory_space=pltpu.SMEM)] + [anywhere] * 5,
        out_specs=(anywhere,) * 5,
        scratch_shapes=[
            vmem((count, width), BF16),
            vmem((width, rows), BF16),
            vmem((count, width), BF16),
            vmem((units, width), BF16),
            vmem((units, width), BF16),
            vmem((blocks, rows, LANES), F32),
            vmem((experts * msg, LANES), F32),
            vmem((4, experts, msg, LANES), BF16),
            vmem((4, experts, msg, LANES), BF16),
            vmem((rows, width), BF16),
            vmem((rows, width), BF16),
            vmem((n_dp + 1, rows, half), BF16),
            vmem((n_dp + 1, rows, half), BF16),
            vmem((n_dp, rows, half), F32),
            vmem((4, rows, width), BF16),
            vmem((count, width), BF16),
            vmem((count, width), BF16),
            vmem((blocks, rows, LANES), F32),
            vmem((width, rows), F32),
            vmem((half, width), BF16),
            vmem((half, width), BF16),
            vmem((n_dp, experts * piece, LANES), F32),
            vmem((n_all, piece, LANES), BF16),
            vmem((n_all, piece, LANES), BF16),
            vmem((piece, LANES), BF16),
            vmem((n_all, piece, LANES), BF16),
            pltpu.SemaphoreType.DMA((5,)),
            pltpu.SemaphoreType.DMA((5,)),
            pltpu.SemaphoreType.DMA((4,)),
            pltpu.SemaphoreType.DMA((4,)),
            pltpu.SemaphoreType.DMA((6,)),
            pltpu.SemaphoreType.DMA((6,)),
        ],
        compiler_params=pltpu.CompilerParams(
            collective_id=0, has_side_effects=True, vmem_limit_bytes=56 << 20
        ),
        name="moe_layer",
    )(slot_count, tokens, phi, grad_out, w_in, w_out)


def solution(mesh):
    both = P(("dp", "expert"), None)
    return jax.shard_map(
        functools.partial(local, mesh.shape["dp"]),
        mesh=mesh,
        in_specs=(both, P(), P(), P("expert", None, None), P("expert", None, None), both),
        out_specs=(both, both, P(), P("expert", "dp", None), P("expert", "dp", None)),
        check_vma=False,
    )
```

```python
import functools
import math

import jax
import jax.numpy as jnp
from jax import lax
from jax.experimental import pallas as pl
from jax.experimental.pallas import tpu as pltpu
from jax.sharding import PartitionSpec as P

LANES = 128
TILE = 16
VMEM_BYTES = 60 * 1024 * 1024
VMEM_SPARE = 48 * 1024
SQRT_HALF = 0.7071067811865476
INV_SQRT_TAU = 0.3989422804014327
MESH = pl.DeviceIdType.MESH
BF16 = jnp.bfloat16
F32 = jnp.float32


def contract(left, right, left_dim, right_dim):
    return lax.dot_general(
        left, right, (((left_dim,), (right_dim,)), ((), ())), preferred_element_type=F32
    )


def softmax_along(logits, axis):
    maximum = jnp.max(logits, axis=axis, keepdims=True)
    weights = jnp.exp(logits - maximum)
    return weights / jnp.sum(weights, axis=axis, keepdims=True)


def kernel(
    dims,
    count_hbm, x_hbm, phi_hbm, g_hbm, win_hbm, wout_hbm,
    mixed_v, gtok_v, gphi_v, gwin_v, gwout_v,
    count_ref, x_v, phi_v, g_v, win_v, wout_v,
    slot_f, pack_f, send_b, recv_b,
    rows_b, cots_b, hid_b, pre_b, slope_f,
    slots_v, gphi_f,
    rs_f, rs_send, rs_recv, ag_own, ag_recv,
    load_sem, swap_send, swap_recv, send_sem, recv_sem,
):
    n_dp, experts, most, blocks, msg, piece = dims
    my_dp = lax.axis_index("dp")
    me = lax.axis_index("expert")
    flat = my_dp * experts + me
    n_all = n_dp * experts
    rows = experts * most
    half = win_v.shape[0] // n_dp
    share = blocks // n_dp

    def lane(k):
        return slice(k * LANES, (k + 1) * LANES)

    def load(src, dst, i):
        return pltpu.make_async_copy(src, dst, load_sem.at[i])

    x_in, phi_in, g_in = load(x_hbm, x_v, 0), load(phi_hbm, phi_v, 1), load(g_hbm, g_v, 2)
    win_in, wout_in = load(win_hbm.at[0], win_v, 3), load(wout_hbm.at[0], wout_v, 4)
    x_in.start()
    phi_in.start()
    g_in.start()
    count_in = load(count_hbm, count_ref, 5)
    count_in.start()

    barrier = pltpu.get_barrier_semaphore()

    @pl.loop(1, n_all)
    def _(t):
        to = lax.rem(flat + t, n_all)
        pl.semaphore_signal(
            barrier, inc=1, device_id=(lax.div(to, experts), lax.rem(to, experts)),
            device_id_type=MESH,
        )

    pack_f[...] = jnp.zeros_like(pack_f)
    rs_f[...] = jnp.zeros_like(rs_f)

    def to_experts(phase):
        for k in range(blocks):
            for j in range(most):
                pack_f[pl.ds(j * blocks + k, experts, stride=msg), :] = slot_f[
                    k, pl.ds(j, experts, stride=most), :
                ]
        ship(phase)

    def to_images(phase, values):
        for k in range(blocks):
            for j in range(most):
                pack_f[pl.ds(j * blocks + k, experts, stride=msg), :] = values[
                    j * experts:(j + 1) * experts, lane(k)
                ]
        ship(phase)

    def ship(phase):
        send_b[phase] = pack_f[...].astype(BF16).reshape(experts, msg, LANES)
        recv_b[phase, me] = send_b[phase, me]

        @pl.loop(1, experts)
        def _(t):
            to = lax.rem(me + t, experts)
            pltpu.make_async_remote_copy(
                src_ref=send_b.at[phase, to],
                dst_ref=recv_b.at[phase, me],
                send_sem=send_sem.at[phase],
                recv_sem=recv_sem.at[phase],
                device_id=(my_dp, to),
                device_id_type=MESH,
            ).start()

    def wait_bytes(ref, sem):
        pltpu.make_async_copy(ref, ref, sem).wait()

    def arrive(phase):
        wait_bytes(recv_b.at[phase, pl.ds(0, experts - 1)], recv_sem.at[phase])
        pack_f[...] = recv_b[phase].astype(F32).reshape(experts * msg, LANES)

    def at_expert(phase, dst):
        arrive(phase)
        for k in range(blocks):
            for j in range(most):
                dst[j * experts:(j + 1) * experts, lane(k)] = pack_f[
                    pl.ds(j * blocks + k, experts, stride=msg), :
                ].astype(BF16)

    def at_image(phase, which):
        arrive(phase)
        for k in range(blocks):
            for j in range(most):
                slot_f[k, pl.ds(j, experts, stride=most), :] = pack_f[
                    pl.ds(j * blocks + k, experts, stride=msg), :
                ]
            slots_v[which, :, lane(k)] = slot_f[k].astype(BF16)

    x_in.wait()
    phi_in.wait()
    x = x_v[...]
    logits = contract(x, phi_v[...], 1, 1)
    spread = softmax_along(logits, 0)
    spread_b = spread.astype(BF16)
    slot_in = contract(spread_b, x, 0, 0)
    for k in range(blocks):
        slot_f[k] = slot_in[:, lane(k)]
    pl.semaphore_wait(barrier, n_all - 1)
    to_experts(0)

    g_in.wait()
    win_in.start()
    wout_in.start()
    count_in.wait()
    column = lax.broadcasted_iota(jnp.int32, (1, rows), 1)
    limit = jnp.zeros((1, rows), jnp.int32)
    for e in range(experts):
        limit = jnp.where(column >= e * most, e * most + count_ref[e], limit)
    live = column < limit
    mixing = softmax_along(jnp.where(live, logits, -1e30), 1)
    mixing_b = mixing.astype(BF16)
    slot_cot = contract(mixing_b, g_v[...], 0, 0)
    for k in range(blocks):
        slot_f[k] = slot_cot[:, lane(k)]
    to_experts(1)

    win_in.wait()
    at_expert(0, rows_b)
    wout_in.wait()
    slot_rows = rows_b[...]
    values = None
    for h in range(n_dp):
        span = slice(h * half, (h + 1) * half)
        preact = contract(slot_rows, win_v[span], 1, 1)
        cdf = 0.5 * (1.0 + lax.erf(preact * SQRT_HALF))
        density = jnp.exp(-0.5 * preact * preact) * INV_SQRT_TAU
        hidden = (preact * cdf).astype(BF16)
        slope_f[h] = cdf + preact * density
        hid_b[h] = hidden
        part = jnp.dot(hidden, wout_v[span], preferred_element_type=F32)
        values = part if values is None else values + part
    to_images(2, values)

    at_expert(1, cots_b)
    cot_rows = cots_b[...]
    grads = None
    for h in range(n_dp):
        span = slice(h * half, (h + 1) * half)
        d_hidden = contract(cot_rows, wout_v[span], 1, 1)
        grad_pre = (d_hidden * slope_f[h]).astype(BF16)
        pre_b[h] = grad_pre
        part = jnp.dot(grad_pre, win_v[span], preferred_element_type=F32)
        grads = part if grads is None else grads + part
    to_images(3, grads)

    other = 1 - my_dp

    def swap(src, dst, i):
        return pltpu.make_async_remote_copy(
            src_ref=src, dst_ref=dst, send_sem=swap_send.at[i], recv_sem=swap_recv.at[i],
            device_id=(other, me), device_id_type=MESH,
        )

    swaps = (
        swap(hid_b.at[other], hid_b.at[n_dp], 0),
        swap(pre_b.at[other], pre_b.at[n_dp], 1),
        swap(rows_b, slots_v.at[2], 2),
        swap(cots_b, slots_v.at[3], 3),
    )
    for copy in swaps:
        copy.start()

    at_image(2, 0)
    slot_values = slots_v[0]
    d_mix = contract(g_v[...], slot_values, 1, 1)
    d_comb = mixing * (d_mix - jnp.sum(d_mix * mixing, axis=1, keepdims=True))
    mixed_v[...] = jnp.dot(mixing_b, slot_values, preferred_element_type=F32).astype(BF16)

    for copy in swaps:
        copy.wait()
    for left, right, theirs, out in (
        (pre_b, rows_b, slots_v.at[2], gwin_v),
        (hid_b, cots_b, slots_v.at[3], gwout_v),
    ):
        mine, given = left[my_dp], left[n_dp]
        out[0] = (
            contract(mine, right[...], 0, 0) + contract(given, theirs[...], 0, 0)
        ).astype(BF16)

    at_image(3, 1)
    slot_grads = slots_v[1]
    d_spread = contract(x_v[...], slot_grads, 1, 1)
    d_disp = spread * (d_spread - jnp.sum(d_spread * spread, axis=0, keepdims=True))
    d_logits = (d_comb + d_disp).astype(BF16)
    term = contract(d_logits, x_v[...], 0, 0)

    for k in range(blocks):
        slot_f[k] = term[:, lane(k)]
    for k in range(blocks):
        for j in range(most):
            rs_f[k // share, pl.ds(j * share + k % share, experts, stride=piece), :] = slot_f[
                k, pl.ds(j, experts, stride=most), :
            ]
    rs_send[...] = rs_f[...].astype(BF16).reshape(n_all, piece, LANES)
    rs_recv[flat] = rs_send[flat]

    def to_all(src_of, dst, i):
        @pl.loop(1, n_all)
        def _(t):
            to = lax.rem(flat + t, n_all)
            pltpu.make_async_remote_copy(
                src_ref=src_of(to), dst_ref=dst.at[flat],
                send_sem=send_sem.at[i], recv_sem=recv_sem.at[i],
                device_id=(lax.div(to, experts), lax.rem(to, experts)),
                device_id_type=MESH,
            ).start()

    to_all(lambda to: rs_send.at[to], rs_recv, 4)

    gtok_v[...] = (
        jnp.dot(d_logits, phi_v[...], preferred_element_type=F32)
        + jnp.dot(spread_b, slot_grads, preferred_element_type=F32)
    ).astype(BF16)

    wait_bytes(rs_recv.at[pl.ds(0, n_all - 1)], recv_sem.at[4])
    ag_own[...] = jnp.sum(rs_recv[...].astype(F32), axis=0).astype(BF16)
    ag_recv[flat] = ag_own[...]
    to_all(lambda to: ag_own, ag_recv, 5)
    wait_bytes(ag_recv.at[pl.ds(0, n_all - 1)], recv_sem.at[5])
    rs_f[...] = ag_recv[...].astype(F32).reshape(n_dp, experts * piece, LANES)
    for k in range(blocks):
        for j in range(most):
            gphi_f[k, pl.ds(j, experts, stride=most), :] = rs_f[
                k // share, pl.ds(j * share + k % share, experts, stride=piece), :
            ]
        gphi_v[:, lane(k)] = gphi_f[k]

    for phase in range(4):
        wait_bytes(send_b.at[phase, pl.ds(0, experts - 1)], send_sem.at[phase])
    wait_bytes(rs_send.at[pl.ds(0, n_all - 1)], send_sem.at[4])
    wait_bytes(ag_recv.at[pl.ds(0, n_all - 1)], send_sem.at[5])


def put_out(*refs):
    sem = refs[-1]
    copies = [
        pltpu.make_async_copy(refs[i], refs[i + 5], sem.at[i]) for i in (3, 4, 0, 1, 2)
    ]
    for copy in copies:
        copy.start()
    for copy in copies:
        copy.wait()


def local(n_dp, tokens, phi, slot_count, w_in, w_out, grad_out):
    experts = slot_count.shape[0]
    count, width = tokens.shape
    units = w_in.shape[1]
    rows = phi.shape[1]
    phi_rows = phi.T
    most = rows // experts
    blocks = width // LANES
    msg = -(-most * blocks // TILE) * TILE
    piece = -(-most * (blocks // n_dp) // TILE) * TILE
    half = units // n_dp
    n_all = n_dp * experts
    dims = (n_dp, experts, most, blocks, msg, piece)
    in_hbm = pl.BlockSpec(memory_space=pltpu.HBM)
    vmem = pltpu.VMEM
    out_shape = (
        jax.ShapeDtypeStruct((count, width), BF16),
        jax.ShapeDtypeStruct((count, width), BF16),
        jax.ShapeDtypeStruct((rows, width), F32),
        jax.ShapeDtypeStruct((1, half, width), BF16),
        jax.ShapeDtypeStruct((1, half, width), BF16),
    )
    staged_bytes = sum(math.prod(o.shape) * o.dtype.itemsize for o in out_shape)
    grant = 40 << 20
    staged = pl.pallas_call(
        functools.partial(kernel, dims),
        out_shape=out_shape,
        in_specs=[in_hbm] * 6,
        out_specs=(pl.BlockSpec(memory_space=vmem),) * 5,
        scratch_shapes=[
            pltpu.SMEM((experts,), jnp.int32),
            vmem((count, width), BF16),
            vmem((rows, width), BF16),
            vmem((count, width), BF16),
            vmem((units, width), BF16),
            vmem((units, width), BF16),
            vmem((blocks, rows, LANES), F32),
            vmem((experts * msg, LANES), F32),
            vmem((4, experts, msg, LANES), BF16),
            vmem((4, experts, msg, LANES), BF16),
            vmem((rows, width), BF16),
            vmem((rows, width), BF16),
            vmem((n_dp + 1, rows, half), BF16),
            vmem((n_dp + 1, rows, half), BF16),
            vmem((n_dp, rows, half), F32),
            vmem((4, rows, width), BF16),
            vmem((blocks, rows, LANES), F32),
            vmem((n_dp, experts * piece, LANES), F32),
            vmem((n_all, piece, LANES), BF16),
            vmem((n_all, piece, LANES), BF16),
            vmem((piece, LANES), BF16),
            vmem((n_all, piece, LANES), BF16),
            pltpu.SemaphoreType.DMA((6,)),
            pltpu.SemaphoreType.DMA((4,)),
            pltpu.SemaphoreType.DMA((4,)),
            pltpu.SemaphoreType.DMA((6,)),
            pltpu.SemaphoreType.DMA((6,)),
        ],
        compiler_params=pltpu.CompilerParams(
            collective_id=0, has_side_effects=True, vmem_limit_bytes=grant
        ),
        name="moe_layer",
    )(*(pltpu.with_memory_space_constraint(a, pltpu.HBM) for a in (slot_count, tokens, phi_rows, grad_out, w_in, w_out)))
    mixed, grad_tokens, grad_phi, grad_in, grad_second = pl.pallas_call(
        put_out,
        out_shape=out_shape,
        in_specs=[pl.BlockSpec(memory_space=vmem)] * 5,
        out_specs=(in_hbm,) * 5,
        scratch_shapes=[pltpu.SemaphoreType.DMA((5,))],
        compiler_params=pltpu.CompilerParams(vmem_limit_bytes=1 << 20),
        name="put_out",
    )(*staged)
    return mixed, grad_tokens, grad_phi.T, grad_in, grad_second


def solution(mesh):
    both = P(("dp", "expert"), None)
    return jax.shard_map(
        functools.partial(local, mesh.shape["dp"]),
        mesh=mesh,
        in_specs=(both, P(), P(), P("expert", None, None), P("expert", None, None), both),
        out_specs=(both, both, P(), P("expert", "dp", None), P("expert", "dp", None)),
        check_vma=False,
    )
```

```python
import functools
import math

import jax
import jax.numpy as jnp
from jax import lax
from jax.experimental import pallas as pl
from jax.experimental.pallas import tpu as pltpu
from jax.sharding import PartitionSpec as P

LANES = 128
TILE = 16
TURN = 256
PARTS = 2
VMEM_OVER = 1.36
SQRT_HALF = 0.7071067811865476
INV_SQRT_TAU = 0.3989422804014327
MESH = pl.DeviceIdType.MESH
BF16 = jnp.bfloat16
F32 = jnp.float32


def contract(left, right, left_dim, right_dim):
    return lax.dot_general(
        left, right, (((left_dim,), (right_dim,)), ((), ())), preferred_element_type=F32
    )


def softmax_along(logits, axis):
    maximum = jnp.max(logits, axis=axis, keepdims=True)
    weights = jnp.exp(logits - maximum)
    return weights / jnp.sum(weights, axis=axis, keepdims=True)


def kernel(
    dims,
    count_hbm, x_hbm, phi_hbm, g_hbm, win_hbm, wout_hbm,
    mixed_v, gtok_v, gphi_v, gwin_v, gwout_v,
    count_ref, x_v, phi_v, g_v, win_v, wout_v, win_t, wout_t,
    slot_f, pack_f, send_b, recv_b,
    rows_b, cots_b, hid_b, pre_b, slope_f,
    slots_v, gphi_f,
    rs_f, rs_in, rs_send, rs_recv, ag_own, ag_recv,
    load_sem, swap_send, swap_recv, send_sem, recv_sem,
):
    n_dp, experts, most, blocks, parts, msg, piece = dims
    my_dp = lax.axis_index("dp")
    me = lax.axis_index("expert")
    flat = my_dp * experts + me
    n_all = n_dp * experts
    rows = experts * most
    half = win_v.shape[0] // n_dp
    share = blocks // n_dp
    per = blocks // parts
    wides = [slice(p * per * LANES, (p + 1) * per * LANES) for p in range(parts)]

    def lane(k):
        return slice(k * LANES, (k + 1) * LANES)

    def load(src, dst, i):
        return pltpu.make_async_copy(src, dst, load_sem.at[i])

    x_in, phi_in, g_in = load(x_hbm, x_v, 0), load(phi_hbm, phi_v, 1), load(g_hbm, g_v, 2)
    win_in, wout_in = load(win_hbm.at[0], win_v, 3), load(wout_hbm.at[0], wout_v, 4)
    x_in.start()
    phi_in.start()
    g_in.start()
    count_in = load(count_hbm, count_ref, 5)
    count_in.start()

    barrier = pltpu.get_barrier_semaphore()

    @pl.loop(1, n_all)
    def _(t):
        to = lax.rem(flat + t, n_all)
        pl.semaphore_signal(
            barrier, inc=1, device_id=(lax.div(to, experts), lax.rem(to, experts)),
            device_id_type=MESH,
        )

    pack_f[...] = jnp.zeros_like(pack_f)
    rs_f[...] = jnp.zeros_like(rs_f)

    steps = [(1 - 2 * lax.rem(lax.div(me, 1 << b), 2)) << b for b in range(experts.bit_length() - 1)]

    def partners(run):
        if experts & (experts - 1) == 0 and experts <= 16:
            for t in range(experts - 1, 0, -1):
                run(me + sum(step for b, step in enumerate(steps) if t >> b & 1))
        else:
            @pl.loop(1, experts)
            def _(t):
                run(lax.rem(me + t, experts))

    def wait_bytes(ref, sem):
        pltpu.make_async_copy(ref, ref, sem).wait()

    def ship(phase, part):
        slot = phase * parts + part
        send_b[slot] = pack_f[...].astype(BF16).reshape(experts, msg, LANES)
        recv_b[slot, me] = send_b[slot, me]

        def run(to):
            pltpu.make_async_remote_copy(
                src_ref=send_b.at[slot, to],
                dst_ref=recv_b.at[slot, me],
                send_sem=send_sem.at[slot],
                recv_sem=recv_sem.at[slot],
                device_id=(my_dp, to),
                device_id_type=MESH,
            ).start()

        partners(run)

    def arrive(phase, part):
        slot = phase * parts + part
        wait_bytes(recv_b.at[slot, pl.ds(0, experts - 1)], recv_sem.at[slot])
        pack_f[...] = recv_b[slot].astype(F32).reshape(experts * msg, LANES)

    def packed(k, j):
        return pl.ds(j * per + k, experts, stride=msg)

    def to_experts(phase, values):
        for part in range(parts):
            for k in range(per):
                slot_f[k] = values[:, lane(part * per + k)]
                for j in range(most):
                    pack_f[packed(k, j), :] = slot_f[k, pl.ds(j, experts, stride=most), :]
            if phase == 0 and part == 0:
                pl.semaphore_wait(barrier, n_all - 1)
            ship(phase, part)

    def to_images(phase, part, values):
        for k in range(per):
            for j in range(most):
                pack_f[packed(k, j), :] = values[j * experts:(j + 1) * experts, lane(k)]
        ship(phase, part)

    def at_expert(phase, part, dst):
        arrive(phase, part)
        for k in range(per):
            for j in range(most):
                dst[j * experts:(j + 1) * experts, lane(part * per + k)] = pack_f[
                    packed(k, j), :
                ].astype(BF16)

    def at_image(phase, which, left):
        product = None
        for part, wide in enumerate(wides):
            arrive(phase, part)
            for k in range(per):
                for j in range(most):
                    slot_f[k, pl.ds(j, experts, stride=most), :] = pack_f[packed(k, j), :]
                slots_v[which, :, lane(part * per + k)] = slot_f[k].astype(BF16)
            term = contract(left[:, wide], slots_v[which, :, wide], 1, 1)
            product = term if product is None else product + term
        return product

    x_in.wait()
    phi_in.wait()
    x = x_v[...]
    logits = contract(x, phi_v[...], 1, 1)
    spread = softmax_along(logits, 0)
    spread_b = spread.astype(BF16)
    slot_in = contract(spread_b, x, 0, 0)
    win_in.start()
    wout_in.start()
    to_experts(0, slot_in)

    g_in.wait()
    count_in.wait()
    column = lax.broadcasted_iota(jnp.int32, (1, rows), 1)
    limit = jnp.zeros((1, rows), jnp.int32)
    for e in range(experts):
        limit = jnp.where(column >= e * most, e * most + count_ref[e], limit)
    live = column < limit
    mixing = softmax_along(jnp.where(live, logits, -1e30), 1)
    mixing_b = mixing.astype(BF16)
    slot_cot = contract(mixing_b, g_v[...], 0, 0)
    to_experts(1, slot_cot)

    def turn(src, dst):
        @pl.loop(0, src.shape[0] // TURN)
        def _(i):
            at = pl.ds(pl.multiple_of(i * TURN, TURN), TURN)
            dst[:, at] = src[at, :].T

    other = 1 - my_dp

    def swap(src, dst, i):
        copy = pltpu.make_async_remote_copy(
            src_ref=src, dst_ref=dst, send_sem=swap_send.at[i], recv_sem=swap_recv.at[i],
            device_id=(other, me), device_id_type=MESH,
        )
        copy.start()
        return copy

    win_in.wait()
    turn(win_v, win_t)
    wout_in.wait()
    turn(wout_v, wout_t)
    for part, wide in enumerate(wides):
        at_expert(0, part, rows_b)
        if part < parts - 1:
            for h in range(n_dp):
                span = slice(h * half, (h + 1) * half)
                term = jnp.dot(rows_b[:, wide], win_t[wide, span], preferred_element_type=F32)
                slope_f[h] = term if part == 0 else slope_f[h] + term
    for h in range(n_dp):
        span = slice(h * half, (h + 1) * half)
        preact = jnp.dot(rows_b[:, wide], win_t[wide, span], preferred_element_type=F32)
        if parts > 1:
            preact = slope_f[h] + preact
        cdf = 0.5 * (1.0 + lax.erf(preact * SQRT_HALF))
        density = jnp.exp(-0.5 * preact * preact) * INV_SQRT_TAU
        slope_f[h] = cdf + preact * density
        hid_b[h] = (preact * cdf).astype(BF16)

    def back_to_images(phase, left, right):
        for part, wide in enumerate(wides):
            total = None
            for h in range(n_dp):
                span = slice(h * half, (h + 1) * half)
                term = jnp.dot(left[h], right[span, wide], preferred_element_type=F32)
                total = term if total is None else total + term
            to_images(phase, part, total)

    back_to_images(2, hid_b, wout_v)

    for part in range(parts):
        at_expert(1, part, cots_b)
    swaps = [
        swap(rows_b, slots_v.at[2], 2),
        swap(cots_b, slots_v.at[3], 3),
        swap(hid_b.at[other], hid_b.at[n_dp], 0),
    ]
    cot_rows = cots_b[...]
    for h in range(n_dp):
        span = slice(h * half, (h + 1) * half)
        d_hidden = jnp.dot(cot_rows, wout_t[:, span], preferred_element_type=F32)
        pre_b[h] = (d_hidden * slope_f[h]).astype(BF16)
    swaps.append(swap(pre_b.at[other], pre_b.at[n_dp], 1))
    back_to_images(3, pre_b, win_v)

    def weight_grad(left, right, theirs, out):
        mine, given = left[my_dp], left[n_dp]
        out[0] = (
            contract(mine, right[...], 0, 0) + contract(given, theirs[...], 0, 0)
        ).astype(BF16)

    for copy in swaps[:3]:
        copy.wait()
    weight_grad(hid_b, cots_b, slots_v.at[3], gwout_v)

    d_mix = at_image(2, 0, g_v)
    d_comb = mixing * (d_mix - jnp.sum(d_mix * mixing, axis=1, keepdims=True))
    d_spread = at_image(3, 1, x_v)
    d_disp = spread * (d_spread - jnp.sum(d_spread * spread, axis=0, keepdims=True))
    d_logits = (d_comb + d_disp).astype(BF16)

    def half_term(which, at):
        start = pl.multiple_of(which * share * LANES, LANES)
        term = contract(d_logits, x_v[:, pl.ds(start, share * LANES)], 0, 0)
        for k in range(share):
            slot_f[k] = term[:, lane(k)]
            for j in range(most):
                rs_f[at, pl.ds(j * share + k, experts, stride=piece), :] = slot_f[
                    k, pl.ds(j, experts, stride=most), :
                ]

    half_term(other, 0)
    given_half = swap(rs_f.at[0], rs_in, 4)
    half_term(my_dp, 1)
    given_half.wait()
    rs_send[...] = (rs_f[1] + rs_in[...]).astype(BF16).reshape(experts, piece, LANES)
    rs_recv[me] = rs_send[me]

    def hand_out(src, dst, at, slot, dp, to):
        pltpu.make_async_remote_copy(
            src_ref=src, dst_ref=dst.at[at], send_sem=send_sem.at[slot],
            recv_sem=recv_sem.at[slot], device_id=(dp, to), device_id_type=MESH,
        ).start()

    partners(lambda to: hand_out(rs_send.at[to], rs_recv, me, 4 * parts, my_dp, to))

    slot_values, slot_grads = slots_v[0], slots_v[1]
    mixed_v[...] = jnp.dot(mixing_b, slot_values, preferred_element_type=F32).astype(BF16)
    gtok_v[...] = (
        jnp.dot(d_logits, phi_v[...], preferred_element_type=F32)
        + jnp.dot(spread_b, slot_grads, preferred_element_type=F32)
    ).astype(BF16)
    swaps[3].wait()
    weight_grad(pre_b, rows_b, slots_v.at[2], gwin_v)

    wait_bytes(rs_recv.at[pl.ds(0, experts - 1)], recv_sem.at[4 * parts])
    ag_own[...] = jnp.sum(rs_recv[...].astype(F32), axis=0).astype(BF16)
    ag_recv[flat] = ag_own[...]

    def to_chip(to):
        hand_out(ag_own, ag_recv, flat, 4 * parts + 1, my_dp, to)
        hand_out(ag_own, ag_recv, flat, 4 * parts + 1, other, to)

    partners(to_chip)
    hand_out(ag_own, ag_recv, flat, 4 * parts + 1, other, me)
    wait_bytes(ag_recv.at[pl.ds(0, n_all - 1)], recv_sem.at[4 * parts + 1])
    rs_f[...] = ag_recv[...].astype(F32).reshape(n_dp, experts * piece, LANES)
    for k in range(blocks):
        for j in range(most):
            gphi_f[k, pl.ds(j, experts, stride=most), :] = rs_f[
                k // share, pl.ds(j * share + k % share, experts, stride=piece), :
            ]
        gphi_v[:, lane(k)] = gphi_f[k]

    for slot in range(4 * parts):
        wait_bytes(send_b.at[slot, pl.ds(0, experts - 1)], send_sem.at[slot])
    wait_bytes(rs_send.at[pl.ds(0, experts - 1)], send_sem.at[4 * parts])
    wait_bytes(ag_recv.at[pl.ds(0, n_all - 1)], send_sem.at[4 * parts + 1])


def put_out(*refs):
    sem = refs[-1]
    copies = [
        pltpu.make_async_copy(refs[i], refs[i + 5], sem.at[i]) for i in (3, 4, 0, 1, 2)
    ]
    for copy in copies:
        copy.start()
    for copy in copies:
        copy.wait()


def local(n_dp, tokens, phi, slot_count, w_in, w_out, grad_out):
    experts = slot_count.shape[0]
    count, width = tokens.shape
    units = w_in.shape[1]
    rows = phi.shape[1]
    phi_rows = phi.T
    most = rows // experts
    blocks = width // LANES
    parts = PARTS
    msg = -(-most * (blocks // parts) // TILE) * TILE
    piece = -(-most * (blocks // n_dp) // TILE) * TILE
    half = units // n_dp
    n_all = n_dp * experts
    dims = (n_dp, experts, most, blocks, parts, msg, piece)
    in_hbm = pl.BlockSpec(memory_space=pltpu.HBM)
    vmem = pltpu.VMEM
    out_shape = (
        jax.ShapeDtypeStruct((count, width), BF16),
        jax.ShapeDtypeStruct((count, width), BF16),
        jax.ShapeDtypeStruct((rows, width), F32),
        jax.ShapeDtypeStruct((1, half, width), BF16),
        jax.ShapeDtypeStruct((1, half, width), BF16),
    )
    scratch = [
        pltpu.SMEM((experts,), jnp.int32),
        vmem((count, width), BF16),
        vmem((rows, width), BF16),
        vmem((count, width), BF16),
        vmem((units, width), BF16),
        vmem((units, width), BF16),
        vmem((width, units), BF16),
        vmem((width, units), BF16),
        vmem((blocks, rows, LANES), F32),
        vmem((experts * msg, LANES), F32),
        vmem((4 * parts, experts, msg, LANES), BF16),
        vmem((4 * parts, experts, msg, LANES), BF16),
        vmem((rows, width), BF16),
        vmem((rows, width), BF16),
        vmem((n_dp + 1, rows, half), BF16),
        vmem((n_dp + 1, rows, half), BF16),
        vmem((n_dp, rows, half), F32),
        vmem((4, rows, width), BF16),
        vmem((blocks, rows, LANES), F32),
        vmem((n_dp, experts * piece, LANES), F32),
        vmem((experts * piece, LANES), F32),
        vmem((experts, piece, LANES), BF16),
        vmem((experts, piece, LANES), BF16),
        vmem((piece, LANES), BF16),
        vmem((n_all, piece, LANES), BF16),
        pltpu.SemaphoreType.DMA((6,)),
        pltpu.SemaphoreType.DMA((5,)),
        pltpu.SemaphoreType.DMA((5,)),
        pltpu.SemaphoreType.DMA((4 * parts + 2,)),
        pltpu.SemaphoreType.DMA((4 * parts + 2,)),
    ]
    held = sum(math.prod(s.shape) * jnp.dtype(s.dtype).itemsize for s in scratch[1:-6])
    staged = pl.pallas_call(
        functools.partial(kernel, dims),
        out_shape=out_shape,
        in_specs=[in_hbm] * 6,
        out_specs=(pl.BlockSpec(memory_space=vmem),) * 5,
        scratch_shapes=scratch,
        compiler_params=pltpu.CompilerParams(
            collective_id=0, has_side_effects=True, vmem_limit_bytes=int(held * VMEM_OVER)
        ),
        name="moe_layer",
    )(*(
        pltpu.with_memory_space_constraint(a, pltpu.HBM)
        for a in (slot_count, tokens, phi_rows, grad_out, w_in, w_out)
    ))
    mixed, grad_tokens, grad_phi, grad_in, grad_second = pl.pallas_call(
        put_out,
        out_shape=out_shape,
        in_specs=[pl.BlockSpec(memory_space=vmem)] * 5,
        out_specs=(in_hbm,) * 5,
        scratch_shapes=[pltpu.SemaphoreType.DMA((5,))],
        compiler_params=pltpu.CompilerParams(vmem_limit_bytes=1 << 20),
        name="put_out",
    )(*staged)
    return mixed, grad_tokens, grad_phi.T, grad_in, grad_second


def solution(mesh):
    both = P(("dp", "expert"), None)
    return jax.shard_map(
        functools.partial(local, mesh.shape["dp"]),
        mesh=mesh,
        in_specs=(both, P(), P(), P("expert", None, None), P("expert", None, None), both),
        out_specs=(both, both, P(), P("expert", "dp", None), P("expert", "dp", None)),
        check_vma=False,
    )
```

```python
import functools
import math

import jax
import jax.numpy as jnp
from jax import lax
from jax.experimental import pallas as pl
from jax.experimental.pallas import tpu as pltpu
from jax.sharding import PartitionSpec as P

LANES = 128
TILE = 16
TURN = 256
PARTS = 2
VMEM_OVER = 1.36
SQRT_HALF = 0.7071067811865476
INV_SQRT_TAU = 0.3989422804014327
MESH = pl.DeviceIdType.MESH
BF16 = jnp.bfloat16
F32 = jnp.float32


def contract(left, right, left_dim, right_dim):
    return lax.dot_general(
        left, right, (((left_dim,), (right_dim,)), ((), ())), preferred_element_type=F32
    )


def softmax_along(logits, axis):
    maximum = jnp.max(logits, axis=axis, keepdims=True)
    weights = jnp.exp(logits - maximum)
    return weights / jnp.sum(weights, axis=axis, keepdims=True)


def kernel(
    dims,
    count_hbm, x_hbm, phi_hbm, g_hbm, win_hbm, wout_hbm,
    mixed_v, gtok_v, gphi_v, gwin_v, gwout_v,
    count_ref, x_v, phi_v, g_v, win_v, wout_v, win_t, wout_t,
    slot_f, pack_f, send_b, recv_b,
    rows_b, cots_b, hid_b, pre_b, slope_f, d_hid_f,
    slots_v, gphi_f,
    rs_f, rs_in, rs_send, rs_recv, ag_own, ag_recv,
    load_sem, swap_send, swap_recv, send_sem, recv_sem,
):
    n_dp, experts, most, blocks, parts, msg, piece = dims
    my_dp = lax.axis_index("dp")
    me = lax.axis_index("expert")
    flat = my_dp * experts + me
    n_all = n_dp * experts
    rows = experts * most
    half = win_v.shape[0] // n_dp
    share = blocks // n_dp
    per = blocks // parts
    wides = [slice(p * per * LANES, (p + 1) * per * LANES) for p in range(parts)]

    barrier = pltpu.get_barrier_semaphore()
    other = 1 - my_dp

    steps = [(1 - 2 * lax.rem(lax.div(me, 1 << b), 2)) << b for b in range(experts.bit_length() - 1)]

    def partners(run):
        if experts & (experts - 1) == 0 and experts <= 16:
            for t in range(experts - 1, 0, -1):
                run(me + sum(step for b, step in enumerate(steps) if t >> b & 1))
        else:
            @pl.loop(1, experts)
            def _(t):
                run(lax.rem(me + t, experts))

    def greet(dp, to):
        pl.semaphore_signal(barrier, inc=1, device_id=(dp, to), device_id_type=MESH)

    def greet_chip(to):
        greet(my_dp, to)
        greet(other, to)

    partners(greet_chip)
    greet(other, me)

    def lane(k):
        return slice(k * LANES, (k + 1) * LANES)

    def load(src, dst, i):
        return pltpu.make_async_copy(src, dst, load_sem.at[i])

    x_in, phi_in, g_in = load(x_hbm, x_v, 0), load(phi_hbm, phi_v, 1), load(g_hbm, g_v, 2)
    win_in, wout_in = load(win_hbm.at[0], win_v, 3), load(wout_hbm.at[0], wout_v, 4)
    x_in.start()
    phi_in.start()
    g_in.start()
    count_in = load(count_hbm, count_ref, 5)
    count_in.start()

    pack_f[...] = jnp.zeros_like(pack_f)
    rs_f[...] = jnp.zeros_like(rs_f)

    def wait_bytes(ref, sem):
        pltpu.make_async_copy(ref, ref, sem).wait()

    def fill(phase, part):
        send_b[phase * parts + part] = pack_f[...].astype(BF16).reshape(experts, msg, LANES)

    def ship(phase, part):
        slot = phase * parts + part

        def run(to):
            pltpu.make_async_remote_copy(
                src_ref=send_b.at[slot, to],
                dst_ref=recv_b.at[slot, me],
                send_sem=send_sem.at[slot],
                recv_sem=recv_sem.at[slot],
                device_id=(my_dp, to),
                device_id_type=MESH,
            ).start()

        partners(run)
        recv_b[slot, me] = send_b[slot, me]

    def arrive(phase, part):
        slot = phase * parts + part
        wait_bytes(recv_b.at[slot, pl.ds(0, experts - 1)], recv_sem.at[slot])
        pack_f[...] = recv_b[slot].astype(F32).reshape(experts * msg, LANES)

    def packed(k, j):
        return pl.ds(j * per + k, experts, stride=msg)

    def to_experts(phase, values):
        for part in range(parts):
            for k in range(per):
                slot_f[k] = values[:, lane(part * per + k)]
                for j in range(most):
                    pack_f[packed(k, j), :] = slot_f[k, pl.ds(j, experts, stride=most), :]
            fill(phase, part)

    def to_images(phase, part, values):
        for k in range(per):
            for j in range(most):
                pack_f[packed(k, j), :] = values[j * experts:(j + 1) * experts, lane(k)]
        fill(phase, part)
        ship(phase, part)

    def at_expert(phase, part, dst):
        arrive(phase, part)
        for k in range(per):
            for j in range(most):
                dst[j * experts:(j + 1) * experts, lane(part * per + k)] = pack_f[
                    packed(k, j), :
                ].astype(BF16)

    def at_image(phase, which, left):
        product = None
        for part, wide in enumerate(wides):
            arrive(phase, part)
            for k in range(per):
                for j in range(most):
                    slot_f[k, pl.ds(j, experts, stride=most), :] = pack_f[packed(k, j), :]
                slots_v[which, :, lane(part * per + k)] = slot_f[k].astype(BF16)
            term = contract(left[:, wide], slots_v[which, :, wide], 1, 1)
            product = term if product is None else product + term
        return product

    x_in.wait()
    phi_in.wait()
    win_in.start()
    wout_in.start()
    x = x_v[...]
    logits = contract(x, phi_v[...], 1, 1)
    spread = softmax_along(logits, 0)
    spread_b = spread.astype(BF16)
    slot_in = contract(spread_b, x, 0, 0)
    to_experts(0, slot_in)
    pl.semaphore_wait(barrier, n_all - 1)
    for part in range(parts):
        ship(0, part)

    g_in.wait()
    count_in.wait()
    column = lax.broadcasted_iota(jnp.int32, (1, rows), 1)
    limit = jnp.zeros((1, rows), jnp.int32)
    for e in range(experts):
        limit = jnp.where(column >= e * most, e * most + count_ref[e], limit)
    live = column < limit
    mixing = softmax_along(jnp.where(live, logits, -1e30), 1)
    mixing_b = mixing.astype(BF16)
    slot_cot = contract(mixing_b, g_v[...], 0, 0)
    to_experts(1, slot_cot)
    for part in range(parts):
        ship(1, part)

    def turn(src, dst):
        @pl.loop(0, src.shape[0] // TURN)
        def _(i):
            at = pl.ds(pl.multiple_of(i * TURN, TURN), TURN)
            dst[:, at] = src[at, :].T

    def swap(src, dst, i):
        copy = pltpu.make_async_remote_copy(
            src_ref=src, dst_ref=dst, send_sem=swap_send.at[i], recv_sem=swap_recv.at[i],
            device_id=(other, me), device_id_type=MESH,
        )
        copy.start()
        return copy

    win_in.wait()
    turn(win_v, win_t)
    wout_in.wait()
    turn(wout_v, wout_t)
    for part, wide in enumerate(wides):
        at_expert(0, part, rows_b)
        if part < parts - 1:
            for h in range(n_dp):
                span = slice(h * half, (h + 1) * half)
                term = jnp.dot(rows_b[:, wide], win_t[wide, span], preferred_element_type=F32)
                slope_f[h] = term if part == 0 else slope_f[h] + term
    for h in range(n_dp):
        span = slice(h * half, (h + 1) * half)
        preact = jnp.dot(rows_b[:, wide], win_t[wide, span], preferred_element_type=F32)
        if parts > 1:
            preact = slope_f[h] + preact
        cdf = 0.5 * (1.0 + lax.erf(preact * SQRT_HALF))
        density = jnp.exp(-0.5 * preact * preact) * INV_SQRT_TAU
        slope_f[h] = cdf + preact * density
        hid_b[h] = (preact * cdf).astype(BF16)

    def back_to_images(phase, left, right):
        for part, wide in enumerate(wides):
            total = None
            for h in range(n_dp):
                span = slice(h * half, (h + 1) * half)
                term = jnp.dot(left[h], right[span, wide], preferred_element_type=F32)
                total = term if total is None else total + term
            to_images(phase, part, total)

    back_to_images(2, hid_b, wout_v)

    for part, wide in enumerate(wides):
        at_expert(1, part, cots_b)
        if part < parts - 1:
            for h in range(n_dp):
                span = slice(h * half, (h + 1) * half)
                term = jnp.dot(cots_b[:, wide], wout_t[wide, span], preferred_element_type=F32)
                d_hid_f[h] = term if part == 0 else d_hid_f[h] + term
    swaps = [
        swap(rows_b, slots_v.at[2], 2),
        swap(cots_b, slots_v.at[3], 3),
        swap(hid_b.at[other], hid_b.at[n_dp], 0),
    ]
    for h in range(n_dp):
        span = slice(h * half, (h + 1) * half)
        d_hidden = jnp.dot(cots_b[:, wide], wout_t[wide, span], preferred_element_type=F32)
        if parts > 1:
            d_hidden = d_hid_f[h] + d_hidden
        pre_b[h] = (d_hidden * slope_f[h]).astype(BF16)
    swaps.append(swap(pre_b.at[other], pre_b.at[n_dp], 1))
    back_to_images(3, pre_b, win_v)

    def weight_grad(left, right, theirs, out):
        mine, given = left[my_dp], left[n_dp]
        out[0] = (
            contract(mine, right[...], 0, 0) + contract(given, theirs[...], 0, 0)
        ).astype(BF16)

    for copy in swaps[:3]:
        copy.wait()
    weight_grad(hid_b, cots_b, slots_v.at[3], gwout_v)

    d_mix = at_image(2, 0, g_v)
    d_comb = mixing * (d_mix - jnp.sum(d_mix * mixing, axis=1, keepdims=True))
    d_spread = at_image(3, 1, x_v)
    d_disp = spread * (d_spread - jnp.sum(d_spread * spread, axis=0, keepdims=True))
    d_logits = (d_comb + d_disp).astype(BF16)

    def half_term(which, at):
        start = pl.multiple_of(which * share * LANES, LANES)
        term = contract(d_logits, x_v[:, pl.ds(start, share * LANES)], 0, 0)
        for k in range(share):
            slot_f[k] = term[:, lane(k)]
            for j in range(most):
                rs_f[at, pl.ds(j * share + k, experts, stride=piece), :] = slot_f[
                    k, pl.ds(j, experts, stride=most), :
                ]

    half_term(other, 0)
    given_half = swap(rs_f.at[0], rs_in, 4)
    half_term(my_dp, 1)
    given_half.wait()
    rs_send[...] = (rs_f[1] + rs_in[...]).astype(BF16).reshape(experts, piece, LANES)
    rs_recv[me] = rs_send[me]

    def hand_out(src, dst, at, slot, dp, to):
        pltpu.make_async_remote_copy(
            src_ref=src, dst_ref=dst.at[at], send_sem=send_sem.at[slot],
            recv_sem=recv_sem.at[slot], device_id=(dp, to), device_id_type=MESH,
        ).start()

    partners(lambda to: hand_out(rs_send.at[to], rs_recv, me, 4 * parts, my_dp, to))

    slot_values, slot_grads = slots_v[0], slots_v[1]
    mixed_v[...] = jnp.dot(mixing_b, slot_values, preferred_element_type=F32).astype(BF16)
    gtok_v[...] = (
        jnp.dot(d_logits, phi_v[...], preferred_element_type=F32)
        + jnp.dot(spread_b, slot_grads, preferred_element_type=F32)
    ).astype(BF16)
    swaps[3].wait()
    weight_grad(pre_b, rows_b, slots_v.at[2], gwin_v)

    wait_bytes(rs_recv.at[pl.ds(0, experts - 1)], recv_sem.at[4 * parts])
    ag_own[...] = jnp.sum(rs_recv[...].astype(F32), axis=0).astype(BF16)
    ag_recv[flat] = ag_own[...]

    def to_chip(to):
        hand_out(ag_own, ag_recv, flat, 4 * parts + 1, my_dp, to)
        hand_out(ag_own, ag_recv, flat, 4 * parts + 1, other, to)

    partners(to_chip)
    hand_out(ag_own, ag_recv, flat, 4 * parts + 1, other, me)
    wait_bytes(ag_recv.at[pl.ds(0, n_all - 1)], recv_sem.at[4 * parts + 1])
    rs_f[...] = ag_recv[...].astype(F32).reshape(n_dp, experts * piece, LANES)
    for k in range(blocks):
        for j in range(most):
            gphi_f[k, pl.ds(j, experts, stride=most), :] = rs_f[
                k // share, pl.ds(j * share + k % share, experts, stride=piece), :
            ]
        gphi_v[:, lane(k)] = gphi_f[k]

    for slot in range(4 * parts):
        wait_bytes(send_b.at[slot, pl.ds(0, experts - 1)], send_sem.at[slot])
    wait_bytes(rs_send.at[pl.ds(0, experts - 1)], send_sem.at[4 * parts])
    wait_bytes(ag_recv.at[pl.ds(0, n_all - 1)], send_sem.at[4 * parts + 1])


def put_out(*refs):
    sem = refs[-1]
    copies = [
        pltpu.make_async_copy(refs[i], refs[i + 5], sem.at[i]) for i in (3, 4, 0, 1, 2)
    ]
    for copy in copies:
        copy.start()
    for copy in copies:
        copy.wait()


def local(n_dp, tokens, phi, slot_count, w_in, w_out, grad_out):
    experts = slot_count.shape[0]
    count, width = tokens.shape
    units = w_in.shape[1]
    rows = phi.shape[1]
    phi_rows = phi.T
    most = rows // experts
    blocks = width // LANES
    parts = PARTS
    msg = -(-most * (blocks // parts) // TILE) * TILE
    piece = -(-most * (blocks // n_dp) // TILE) * TILE
    half = units // n_dp
    n_all = n_dp * experts
    dims = (n_dp, experts, most, blocks, parts, msg, piece)
    in_hbm = pl.BlockSpec(memory_space=pltpu.HBM)
    vmem = pltpu.VMEM
    out_shape = (
        jax.ShapeDtypeStruct((count, width), BF16),
        jax.ShapeDtypeStruct((count, width), BF16),
        jax.ShapeDtypeStruct((rows, width), F32),
        jax.ShapeDtypeStruct((1, half, width), BF16),
        jax.ShapeDtypeStruct((1, half, width), BF16),
    )
    scratch = [
        pltpu.SMEM((experts,), jnp.int32),
        vmem((count, width), BF16),
        vmem((rows, width), BF16),
        vmem((count, width), BF16),
        vmem((units, width), BF16),
        vmem((units, width), BF16),
        vmem((width, units), BF16),
        vmem((width, units), BF16),
        vmem((blocks, rows, LANES), F32),
        vmem((experts * msg, LANES), F32),
        vmem((4 * parts, experts, msg, LANES), BF16),
        vmem((4 * parts, experts, msg, LANES), BF16),
        vmem((rows, width), BF16),
        vmem((rows, width), BF16),
        vmem((n_dp + 1, rows, half), BF16),
        vmem((n_dp + 1, rows, half), BF16),
        vmem((n_dp, rows, half), F32),
        vmem((n_dp, rows, half), F32),
        vmem((4, rows, width), BF16),
        vmem((blocks, rows, LANES), F32),
        vmem((n_dp, experts * piece, LANES), F32),
        vmem((experts * piece, LANES), F32),
        vmem((experts, piece, LANES), BF16),
        vmem((experts, piece, LANES), BF16),
        vmem((piece, LANES), BF16),
        vmem((n_all, piece, LANES), BF16),
        pltpu.SemaphoreType.DMA((6,)),
        pltpu.SemaphoreType.DMA((5,)),
        pltpu.SemaphoreType.DMA((5,)),
        pltpu.SemaphoreType.DMA((4 * parts + 2,)),
        pltpu.SemaphoreType.DMA((4 * parts + 2,)),
    ]
    held = sum(math.prod(s.shape) * jnp.dtype(s.dtype).itemsize for s in scratch[1:-6])
    staged = pl.pallas_call(
        functools.partial(kernel, dims),
        out_shape=out_shape,
        in_specs=[in_hbm] * 6,
        out_specs=(pl.BlockSpec(memory_space=vmem),) * 5,
        scratch_shapes=scratch,
        compiler_params=pltpu.CompilerParams(
            collective_id=0, has_side_effects=True, vmem_limit_bytes=int(held * VMEM_OVER)
        ),
        name="moe_layer",
    )(*(
        pltpu.with_memory_space_constraint(a, pltpu.HBM)
        for a in (slot_count, tokens, phi_rows, grad_out, w_in, w_out)
    ))
    mixed, grad_tokens, grad_phi, grad_in, grad_second = pl.pallas_call(
        put_out,
        out_shape=out_shape,
        in_specs=[pl.BlockSpec(memory_space=vmem)] * 5,
        out_specs=(in_hbm,) * 5,
        scratch_shapes=[pltpu.SemaphoreType.DMA((5,))],
        compiler_params=pltpu.CompilerParams(vmem_limit_bytes=1 << 20),
        name="put_out",
    )(*staged)
    return mixed, grad_tokens, grad_phi.T, grad_in, grad_second


def solution(mesh):
    both = P(("dp", "expert"), None)
    return jax.shard_map(
        functools.partial(local, mesh.shape["dp"]),
        mesh=mesh,
        in_specs=(both, P(), P(), P("expert", None, None), P("expert", None, None), both),
        out_specs=(both, both, P(), P("expert", "dp", None), P("expert", "dp", None)),
        check_vma=False,
    )
```

```python
import functools
import math

import jax
import jax.numpy as jnp
from jax import lax
from jax.experimental import pallas as pl
from jax.experimental.pallas import tpu as pltpu
from jax.sharding import PartitionSpec as P

LANES = 128
TILE = 16
TURN = 256
PARTS = 2
VMEM_OVER = 1.36
SQRT_HALF = 0.7071067811865476
INV_SQRT_TAU = 0.3989422804014327
MESH = pl.DeviceIdType.MESH
BF16 = jnp.bfloat16
F32 = jnp.float32


def contract(left, right, left_dim, right_dim):
    return lax.dot_general(
        left, right, (((left_dim,), (right_dim,)), ((), ())), preferred_element_type=F32
    )


def softmax_along(logits, axis):
    maximum = jnp.max(logits, axis=axis, keepdims=True)
    weights = jnp.exp(logits - maximum)
    return weights / jnp.sum(weights, axis=axis, keepdims=True)


def kernel(
    dims,
    count_hbm, x_hbm, phi_hbm, g_hbm, win_hbm, wout_hbm,
    mixed_v, gtok_v, gphi_v, gwin_v, gwout_v,
    count_ref, x_v, phi_v, g_v, win_v, wout_v, win_t, wout_t,
    slot_f, pack_f, send_b, recv_b,
    rows_b, cots_b, hid_b, pre_b, slope_f, d_hid_f,
    slots_v, gphi_f,
    rs_f, rs_in, rs_send, rs_recv, ag_own, ag_recv,
    load_sem, swap_send, swap_recv, send_sem, recv_sem,
):
    n_dp, experts, most, blocks, parts, msg, piece = dims
    my_dp = lax.axis_index("dp")
    me = lax.axis_index("expert")
    flat = my_dp * experts + me
    n_all = n_dp * experts
    rows = experts * most
    half = win_v.shape[0] // n_dp
    share = blocks // n_dp
    per = blocks // parts
    wides = [slice(p * per * LANES, (p + 1) * per * LANES) for p in range(parts)]

    barrier = pltpu.get_barrier_semaphore()
    other = 1 - my_dp

    steps = [(1 - 2 * lax.rem(lax.div(me, 1 << b), 2)) << b for b in range(experts.bit_length() - 1)]

    def partners(run):
        if experts & (experts - 1) == 0 and experts <= 16:
            for t in range(experts - 1, 0, -1):
                run(me + sum(step for b, step in enumerate(steps) if t >> b & 1))
        else:
            @pl.loop(1, experts)
            def _(t):
                run(lax.rem(me + t, experts))

    def greet(dp, to):
        pl.semaphore_signal(barrier, inc=1, device_id=(dp, to), device_id_type=MESH)

    def greet_chip(to):
        greet(my_dp, to)
        greet(other, to)

    partners(greet_chip)
    greet(other, me)

    def lane(k):
        return slice(k * LANES, (k + 1) * LANES)

    def load(src, dst, i):
        return pltpu.make_async_copy(src, dst, load_sem.at[i])

    x_in, phi_in, g_in = load(x_hbm, x_v, 0), load(phi_hbm, phi_v, 1), load(g_hbm, g_v, 2)
    win_in, wout_in = load(win_hbm.at[0], win_v, 3), load(wout_hbm.at[0], wout_v, 4)
    x_in.start()
    phi_in.start()
    g_in.start()
    count_in = load(count_hbm, count_ref, 5)
    count_in.start()

    pack_f[...] = jnp.zeros_like(pack_f)
    rs_f[...] = jnp.zeros_like(rs_f)

    def wait_bytes(ref, sem):
        pltpu.make_async_copy(ref, ref, sem).wait()

    def fill(phase, part):
        send_b[phase * parts + part] = pack_f[...].astype(BF16).reshape(experts, msg, LANES)

    def ship(phase, part):
        slot = phase * parts + part

        def run(to):
            pltpu.make_async_remote_copy(
                src_ref=send_b.at[slot, to],
                dst_ref=recv_b.at[slot, me],
                send_sem=send_sem.at[slot],
                recv_sem=recv_sem.at[slot],
                device_id=(my_dp, to),
                device_id_type=MESH,
            ).start()

        partners(run)
        recv_b[slot, me] = send_b[slot, me]

    def arrive(phase, part):
        slot = phase * parts + part
        wait_bytes(recv_b.at[slot, pl.ds(0, experts - 1)], recv_sem.at[slot])
        pack_f[...] = recv_b[slot].astype(F32).reshape(experts * msg, LANES)

    def packed(k, j):
        return pl.ds(j * per + k, experts, stride=msg)

    def to_experts(phase, values):
        for part in range(parts):
            for k in range(per):
                slot_f[k] = values[:, lane(part * per + k)]
                for j in range(most):
                    pack_f[packed(k, j), :] = slot_f[k, pl.ds(j, experts, stride=most), :]
            fill(phase, part)

    def to_images(phase, part, values):
        for k in range(per):
            for j in range(most):
                pack_f[packed(k, j), :] = values[j * experts:(j + 1) * experts, lane(k)]
        fill(phase, part)
        ship(phase, part)

    def at_expert(phase, part, dst):
        arrive(phase, part)
        for k in range(per):
            for j in range(most):
                dst[j * experts:(j + 1) * experts, lane(part * per + k)] = pack_f[
                    packed(k, j), :
                ].astype(BF16)

    def at_image(phase, which, left):
        product = None
        for part, wide in enumerate(wides):
            arrive(phase, part)
            for k in range(per):
                for j in range(most):
                    slot_f[k, pl.ds(j, experts, stride=most), :] = pack_f[packed(k, j), :]
                slots_v[which, :, lane(part * per + k)] = slot_f[k].astype(BF16)
            term = contract(left[:, wide], slots_v[which, :, wide], 1, 1)
            product = term if product is None else product + term
        return product

    x_in.wait()
    phi_in.wait()
    win_in.start()
    wout_in.start()
    x = x_v[...]
    logits = contract(x, phi_v[...], 1, 1)
    spread = softmax_along(logits, 0)
    spread_b = spread.astype(BF16)
    slot_in = contract(spread_b, x, 0, 0)
    to_experts(0, slot_in)
    pl.semaphore_wait(barrier, n_all - 1)
    for part in range(parts):
        ship(0, part)

    g_in.wait()
    count_in.wait()
    column = lax.broadcasted_iota(jnp.int32, (1, rows), 1)
    limit = jnp.zeros((1, rows), jnp.int32)
    for e in range(experts):
        limit = jnp.where(column >= e * most, e * most + count_ref[e], limit)
    live = column < limit
    mixing = softmax_along(jnp.where(live, logits, -1e30), 1)
    mixing_b = mixing.astype(BF16)
    slot_cot = contract(mixing_b, g_v[...], 0, 0)
    to_experts(1, slot_cot)
    for part in range(parts):
        ship(1, part)

    def turn(src, dst):
        @pl.loop(0, src.shape[0] // TURN)
        def _(i):
            at = pl.ds(pl.multiple_of(i * TURN, TURN), TURN)
            dst[:, at] = src[at, :].T

    def swap(src, dst, i):
        copy = pltpu.make_async_remote_copy(
            src_ref=src, dst_ref=dst, send_sem=swap_send.at[i], recv_sem=swap_recv.at[i],
            device_id=(other, me), device_id_type=MESH,
        )
        copy.start()
        return copy

    win_in.wait()
    turn(win_v, win_t)
    wout_in.wait()
    turn(wout_v, wout_t)
    for part, wide in enumerate(wides):
        at_expert(0, part, rows_b)
        if part < parts - 1:
            for h in range(n_dp):
                span = slice(h * half, (h + 1) * half)
                term = jnp.dot(rows_b[:, wide], win_t[wide, span], preferred_element_type=F32)
                slope_f[h] = term if part == 0 else slope_f[h] + term
    for h in range(n_dp):
        span = slice(h * half, (h + 1) * half)
        preact = jnp.dot(rows_b[:, wide], win_t[wide, span], preferred_element_type=F32)
        if parts > 1:
            preact = slope_f[h] + preact
        cdf = 0.5 * (1.0 + lax.erf(preact * SQRT_HALF))
        density = jnp.exp(-0.5 * preact * preact) * INV_SQRT_TAU
        slope_f[h] = cdf + preact * density
        hid_b[h] = (preact * cdf).astype(BF16)

    def back_to_images(phase, left, right):
        for part, wide in enumerate(wides):
            total = None
            for h in range(n_dp):
                span = slice(h * half, (h + 1) * half)
                term = jnp.dot(left[h], right[span, wide], preferred_element_type=F32)
                total = term if total is None else total + term
            to_images(phase, part, total)

    back_to_images(2, hid_b, wout_v)

    for part, wide in enumerate(wides):
        at_expert(1, part, cots_b)
        if part < parts - 1:
            for h in range(n_dp):
                span = slice(h * half, (h + 1) * half)
                term = jnp.dot(cots_b[:, wide], wout_t[wide, span], preferred_element_type=F32)
                d_hid_f[h] = term if part == 0 else d_hid_f[h] + term
    swaps = [
        swap(rows_b, slots_v.at[2], 2),
        swap(cots_b, slots_v.at[3], 3),
        swap(hid_b.at[other], hid_b.at[n_dp], 0),
    ]
    for h in range(n_dp):
        span = slice(h * half, (h + 1) * half)
        d_hidden = jnp.dot(cots_b[:, wide], wout_t[wide, span], preferred_element_type=F32)
        if parts > 1:
            d_hidden = d_hid_f[h] + d_hidden
        pre_b[h] = (d_hidden * slope_f[h]).astype(BF16)
    swaps.append(swap(pre_b.at[other], pre_b.at[n_dp], 1))
    back_to_images(3, pre_b, win_v)

    def weight_grad(left, right, theirs, out):
        mine, given = left[my_dp], left[n_dp]
        out[0] = (
            contract(mine, right[...], 0, 0) + contract(given, theirs[...], 0, 0)
        ).astype(BF16)

    for copy in swaps[:3]:
        copy.wait()
    weight_grad(hid_b, cots_b, slots_v.at[3], gwout_v)

    d_mix = at_image(2, 0, g_v)
    d_comb = mixing * (d_mix - jnp.sum(d_mix * mixing, axis=1, keepdims=True))
    d_spread = at_image(3, 1, x_v)
    d_disp = spread * (d_spread - jnp.sum(d_spread * spread, axis=0, keepdims=True))
    d_logits = (d_comb + d_disp).astype(BF16)

    def half_term(which, at):
        start = pl.multiple_of(which * share * LANES, LANES)
        term = contract(d_logits, x_v[:, pl.ds(start, share * LANES)], 0, 0)
        for k in range(share):
            slot_f[k] = term[:, lane(k)]
            for j in range(most):
                rs_f[at, pl.ds(j * share + k, experts, stride=piece), :] = slot_f[
                    k, pl.ds(j, experts, stride=most), :
                ]

    half_term(other, 0)
    given_half = swap(rs_f.at[0], rs_in, 4)
    half_term(my_dp, 1)
    given_half.wait()
    rs_send[...] = (rs_f[1] + rs_in[...]).astype(BF16).reshape(experts, piece, LANES)
    rs_recv[me] = rs_send[me]

    def hand_out(src, dst, at, slot, dp, to):
        pltpu.make_async_remote_copy(
            src_ref=src, dst_ref=dst.at[at], send_sem=send_sem.at[slot],
            recv_sem=recv_sem.at[slot], device_id=(dp, to), device_id_type=MESH,
        ).start()

    partners(lambda to: hand_out(rs_send.at[to], rs_recv, me, 4 * parts, my_dp, to))

    slot_values, slot_grads = slots_v[0], slots_v[1]
    mixed_v[...] = jnp.dot(mixing_b, slot_values, preferred_element_type=F32).astype(BF16)
    gtok_v[...] = (
        jnp.dot(d_logits, phi_v[...], preferred_element_type=F32)
        + jnp.dot(spread_b, slot_grads, preferred_element_type=F32)
    ).astype(BF16)
    wait_bytes(rs_recv.at[pl.ds(0, experts - 1)], recv_sem.at[4 * parts])
    ag_own[...] = jnp.sum(rs_recv[...].astype(F32), axis=0).astype(BF16)
    ag_recv[flat] = ag_own[...]

    def to_chip(to):
        hand_out(ag_own, ag_recv, flat, 4 * parts + 1, my_dp, to)
        hand_out(ag_own, ag_recv, flat, 4 * parts + 1, other, to)

    partners(to_chip)
    hand_out(ag_own, ag_recv, flat, 4 * parts + 1, other, me)
    swaps[3].wait()
    weight_grad(pre_b, rows_b, slots_v.at[2], gwin_v)

    wait_bytes(ag_recv.at[pl.ds(0, n_all - 1)], recv_sem.at[4 * parts + 1])
    rs_f[...] = ag_recv[...].astype(F32).reshape(n_dp, experts * piece, LANES)
    for k in range(blocks):
        for j in range(most):
            gphi_f[k, pl.ds(j, experts, stride=most), :] = rs_f[
                k // share, pl.ds(j * share + k % share, experts, stride=piece), :
            ]
        gphi_v[:, lane(k)] = gphi_f[k]

    for slot in range(4 * parts):
        wait_bytes(send_b.at[slot, pl.ds(0, experts - 1)], send_sem.at[slot])
    wait_bytes(rs_send.at[pl.ds(0, experts - 1)], send_sem.at[4 * parts])
    wait_bytes(ag_recv.at[pl.ds(0, n_all - 1)], send_sem.at[4 * parts + 1])


def put_out(*refs):
    sem = refs[-1]
    copies = [
        pltpu.make_async_copy(refs[i], refs[i + 5], sem.at[i]) for i in (3, 4, 0, 1, 2)
    ]
    for copy in copies:
        copy.start()
    for copy in copies:
        copy.wait()


def local(n_dp, tokens, phi, slot_count, w_in, w_out, grad_out):
    experts = slot_count.shape[0]
    count, width = tokens.shape
    units = w_in.shape[1]
    rows = phi.shape[1]
    phi_rows = phi.T
    most = rows // experts
    blocks = width // LANES
    parts = PARTS
    msg = -(-most * (blocks // parts) // TILE) * TILE
    piece = -(-most * (blocks // n_dp) // TILE) * TILE
    half = units // n_dp
    n_all = n_dp * experts
    dims = (n_dp, experts, most, blocks, parts, msg, piece)
    in_hbm = pl.BlockSpec(memory_space=pltpu.HBM)
    vmem = pltpu.VMEM
    out_shape = (
        jax.ShapeDtypeStruct((count, width), BF16),
        jax.ShapeDtypeStruct((count, width), BF16),
        jax.ShapeDtypeStruct((rows, width), F32),
        jax.ShapeDtypeStruct((1, half, width), BF16),
        jax.ShapeDtypeStruct((1, half, width), BF16),
    )
    scratch = [
        pltpu.SMEM((experts,), jnp.int32),
        vmem((count, width), BF16),
        vmem((rows, width), BF16),
        vmem((count, width), BF16),
        vmem((units, width), BF16),
        vmem((units, width), BF16),
        vmem((width, units), BF16),
        vmem((width, units), BF16),
        vmem((blocks, rows, LANES), F32),
        vmem((experts * msg, LANES), F32),
        vmem((4 * parts, experts, msg, LANES), BF16),
        vmem((4 * parts, experts, msg, LANES), BF16),
        vmem((rows, width), BF16),
        vmem((rows, width), BF16),
        vmem((n_dp + 1, rows, half), BF16),
        vmem((n_dp + 1, rows, half), BF16),
        vmem((n_dp, rows, half), F32),
        vmem((n_dp, rows, half), F32),
        vmem((4, rows, width), BF16),
        vmem((blocks, rows, LANES), F32),
        vmem((n_dp, experts * piece, LANES), F32),
        vmem((experts * piece, LANES), F32),
        vmem((experts, piece, LANES), BF16),
        vmem((experts, piece, LANES), BF16),
        vmem((piece, LANES), BF16),
        vmem((n_all, piece, LANES), BF16),
        pltpu.SemaphoreType.DMA((6,)),
        pltpu.SemaphoreType.DMA((5,)),
        pltpu.SemaphoreType.DMA((5,)),
        pltpu.SemaphoreType.DMA((4 * parts + 2,)),
        pltpu.SemaphoreType.DMA((4 * parts + 2,)),
    ]
    held = sum(math.prod(s.shape) * jnp.dtype(s.dtype).itemsize for s in scratch[1:-6])
    staged = pl.pallas_call(
        functools.partial(kernel, dims),
        out_shape=out_shape,
        in_specs=[in_hbm] * 6,
        out_specs=(pl.BlockSpec(memory_space=vmem),) * 5,
        scratch_shapes=scratch,
        compiler_params=pltpu.CompilerParams(
            collective_id=0, has_side_effects=True, vmem_limit_bytes=int(held * VMEM_OVER)
        ),
        name="moe_layer",
    )(*(
        pltpu.with_memory_space_constraint(a, pltpu.HBM)
        for a in (slot_count, tokens, phi_rows, grad_out, w_in, w_out)
    ))
    mixed, grad_tokens, grad_phi, grad_in, grad_second = pl.pallas_call(
        put_out,
        out_shape=out_shape,
        in_specs=[pl.BlockSpec(memory_space=vmem)] * 5,
        out_specs=(in_hbm,) * 5,
        scratch_shapes=[pltpu.SemaphoreType.DMA((5,))],
        compiler_params=pltpu.CompilerParams(vmem_limit_bytes=1 << 20),
        name="put_out",
    )(*staged)
    return mixed, grad_tokens, grad_phi.T, grad_in, grad_second


def solution(mesh):
    both = P(("dp", "expert"), None)
    return jax.shard_map(
        functools.partial(local, mesh.shape["dp"]),
        mesh=mesh,
        in_specs=(both, P(), P(), P("expert", None, None), P("expert", None, None), both),
        out_specs=(both, both, P(), P("expert", "dp", None), P("expert", "dp", None)),
        check_vma=False,
    )
```
